32 devices in a mesh: groups: 2 (over y), expert: 16 (over z, x, core).
Axes of the slice: x: 2, y: 2, z: 4, core: 2. Of those that a mesh axis runs over, the one named last changes fastest.
Arguments:
- tokens: bfloat16 [512, 3584], P(('groups', 'expert')), parts along dimension 0, may hold values from -6 to 6
- live_counts: int32 [32], P(('groups', 'expert')), parts along dimension 0, may hold values from 8 to 16, as said below
- expert_ids: int32 [512, 4], P(('groups', 'expert')), parts along dimension 0, may hold values from 0 to 7, all different within a row; in each aligned block of 16 rows (0 to 15, 16 to 31, ...) at most 16 rows name the same one
- gate_scores: float32 [512, 4], P(('groups', 'expert')), parts along dimension 0, may hold values from 0.1 to 1
- gate_weight: bfloat16 [16, 3584, 512], P('expert'), may hold values from -0.09375 to 0.09375
- up_weight: bfloat16 [16, 3584, 512], P('expert'), may hold values from -0.09375 to 0.09375
- down_weight: bfloat16 [16, 512, 3584], P('expert'), may hold values from -0.1875 to 0.1875
Outputs:
- moe_out: bfloat16 [512, 3584], P(('groups', 'expert')), parts along dimension 0
The draws below stay inside these ranges and needn't reach their ends.
There are 2 independent parts, one for each index of `groups`. The reference program is written for one: setup_inputs(seed, part) draws one part's arguments, and reference() takes and returns one part's arrays. A program takes and returns all parts, laid end to end along the dimension named above; an argument that names none is the same for every part. Nothing has to cross between parts.
Inputs may be any that keep to these rules, and one draw needn't show every extreme that they name: `expert_ids`: A row names 4 different experts. In each device's aligned block of 16 rows no expert is named by more than 16 rows, a bound that some block reaches. `live_counts`: some device has all 16 slots live.
All inputs are finite; a program needn't handle non-finite values.
Results may differ from the reference program's by a relative error of at most 0.0068.
Values may be sent and summed in bfloat16 or wider, within the bound.
A program may use at most 64 MiB of HBM per device.

```python
import math
import jax
import jax.numpy as jnp
import numpy as np
from jax import lax

D = 3584
FF = 1024
TOP = 4
TOK_DEV = 16
FF_HALF = 512
EXPERTS = 8
CAP = 16
TOKENS = 256
N_EXPERT = 16


def draw_live_counts(key, part):
    devices = TOKENS // TOK_DEV
    counts = jax.random.randint(jax.random.fold_in(key, 11), (devices,), TOK_DEV // 2, TOK_DEV + 1)
    full_device = jax.random.randint(jax.random.fold_in(key, 12), (), 0, devices)
    counts = jnp.where(jnp.arange(devices) == full_device, TOK_DEV, counts)
    return counts.astype(jnp.int32)


def block_scale(key, extent, pieces, least, largest):
    level, own = 1.0, jax.random.fold_in(key, 6)
    for dim, shards_of in pieces:
        heights = jnp.exp(jax.random.uniform(jax.random.fold_in(own, dim), (shards_of,), jnp.float32, least / len(pieces), largest / len(pieces)))
        level = level * jnp.repeat(heights, extent[dim] // shards_of).reshape([-1 if axis == dim else 1 for axis in range(len(extent))])
    return level


def shared_out(rng, own, number, rows, amount, top, most, slope):
    order = jax.random.permutation(rng, amount)
    packed, usual = portions_of(amount, rows * top, most, slope, True), portions_of(amount, rows * top, most, slope, False)
    places = jnp.arange(amount)

    def named(sizes, turn):
        used = int((sizes > 0).sum())
        fixed = max(1, used // 4)
        passed = fixed + (places - fixed + turn * (used - fixed)) % max(1, amount - fixed)
        return jnp.zeros((amount,), jnp.int32).at[order[jnp.where(places < fixed, places, passed)]].set(jnp.asarray(sizes, jnp.int32))

    sizes = jnp.where(number % 4 == 0, named(packed, number // 4), named(usual, number - number // 4 - 1))
    mixed = jax.random.permutation(jax.random.fold_in(own, 3), amount)
    giver, receiver = mixed[0:amount // 2 * 2:2], mixed[1:amount // 2 * 2:2]
    margin = jnp.minimum(sizes[giver] - 1, most - sizes[receiver]) // 2
    margin = jnp.where((giver == order[0]) | (receiver == order[0]) | (sizes[receiver] == 0), 0, jnp.maximum(margin, 0))
    passed = jax.random.randint(jax.random.fold_in(own, 4), (amount // 2,), 0, 1 << 20) % (margin + 1)
    sizes = sizes.at[giver].add(-passed).at[receiver].add(passed)
    items = jnp.searchsorted(jnp.cumsum(sizes), jnp.arange(rows * top), side="right").astype(jnp.int32)
    table = items.reshape(top, rows).T
    table = table[jax.random.permutation(jax.random.fold_in(own, 1), rows)]
    turn = jax.random.randint(jax.random.fold_in(own, 2), (rows, 1), 0, top)
    return jnp.take_along_axis(table, (jnp.arange(top)[None, :] + turn) % top, axis=1)


def portions_of(number_of, total, most, lean, full):
    portions = [(1 << 20) // math.isqrt(standing ** lean) + 1 for standing in range(1, number_of + 1)]
    largest = most if full else min(most, max(-(-total // number_of), total * portions[0] // sum(portions)))
    least = 1 if total - largest >= number_of - 1 else 0
    given, surplus = [largest] + [least] * (number_of - 1), total - largest - least * (number_of - 1)
    while surplus > 0:
        candidates = [i for i in range(1, number_of) if given[i] < largest] or [i for i in range(1, number_of) if given[i] < most]
        pool, left = sum([portions[i] for i in candidates]), surplus
        for i in candidates:
            addition = min(most - given[i], max(1, left * portions[i] // pool), surplus)
            given[i] = given[i] + addition
            surplus = surplus - addition
    return np.array(given)


def noise(own_key, extent, width, limit, pieces=(), kind=jnp.bfloat16):
    gain = block_scale(own_key, extent, pieces, -0.22, 0.18) if pieces else 1.0
    result = jax.random.normal(own_key, extent, jnp.float32) * width * gain
    return jnp.minimum(jnp.maximum(result, -limit), limit).astype(kind)


def setup_inputs(seed: int = 0, part: int = 0) -> dict:
    key_list = jax.random.split(jax.random.key(seed), 8)
    part_splits = jax.random.split(jax.random.fold_in(key_list[7], part), 8)
    tokens = noise(part_splits[0], (TOKENS, D), 1.0, 6.0, ((0, 16),))
    live_counts = draw_live_counts(jax.random.fold_in(jax.random.fold_in(key_list[7], part), 71), part)
    expert_ids_keys = jax.random.split(jax.random.fold_in(part_splits[2], 1), TOKENS // TOK_DEV)
    expert_ids_turns = jax.random.permutation(jax.random.fold_in(part_splits[2], 3), TOKENS // TOK_DEV)
    expert_ids = jax.vmap(lambda own, number: shared_out(jax.random.fold_in(part_splits[2], 2), own, number, TOK_DEV, EXPERTS, TOP, CAP, 2))(expert_ids_keys, expert_ids_turns).reshape((TOKENS, TOP))
    gate_scores = jnp.clip(jnp.exp(math.log(1.0) - 2.3025851 * jax.random.uniform(part_splits[3], (TOKENS, TOP), jnp.float32) ** block_scale(part_splits[3], (TOKENS, TOP), ((0, 16),), -0.2, 0.2)), 0.1, 1.0)
    gate_weight = noise(key_list[4], (N_EXPERT, D, FF_HALF), D ** -0.5, 0.09375, ((0, 16),))
    up_weight = noise(key_list[5], (N_EXPERT, D, FF_HALF), D ** -0.5, 0.09375, ((0, 16),))
    down_weight = noise(key_list[6], (N_EXPERT, FF_HALF, D), FF ** -0.5, 0.1875, ((0, 16),))
    return dict(tokens=tokens, live_counts=live_counts, expert_ids=expert_ids, gate_scores=gate_scores, gate_weight=gate_weight, up_weight=up_weight, down_weight=down_weight)


def expert_rows(gate_pair, up_pair, down_pair, inputs):
    gate_full = jnp.concatenate([gate_pair[0], gate_pair[1]], axis=1)
    up_full = jnp.concatenate([up_pair[0], up_pair[1]], axis=1)
    down_full = jnp.concatenate([down_pair[0], down_pair[1]], axis=0)
    gate_act = jnp.dot(inputs, gate_full, preferred_element_type=jnp.float32)
    up_act = jnp.dot(inputs, up_full, preferred_element_type=jnp.float32)
    hidden = (jax.nn.silu(gate_act) * up_act).astype(jnp.bfloat16)
    return jnp.dot(hidden, down_full, preferred_element_type=jnp.float32).astype(jnp.bfloat16)


def reference(tokens, live_counts, expert_ids, gate_scores, gate_weight, up_weight, down_weight):
    devices = N_EXPERT
    block_ids = expert_ids.reshape(devices, TOK_DEV * TOP)
    onehot = (block_ids[:, :, None] == jnp.arange(EXPERTS, dtype=jnp.int32)[None, None, :]).astype(jnp.int32)
    earlier = jnp.cumsum(onehot, axis=1) - onehot
    slot_index = jnp.sum(earlier * onehot, axis=2)
    source = jnp.arange(devices, dtype=jnp.int32)[:, None]
    position = (source * CAP + slot_index).reshape(-1).astype(jnp.int32)
    token_index = jnp.repeat(jnp.arange(TOKENS, dtype=jnp.int32), TOP)
    flat_ids = expert_ids.reshape(-1).astype(jnp.int32)
    slot_table = jnp.full((EXPERTS, devices * CAP), TOKENS, dtype=jnp.int32)
    slot_table = slot_table.at[flat_ids, position].set(token_index)
    padded = jnp.concatenate([tokens, jnp.zeros((1, D), tokens.dtype)], axis=0)

    def one_expert(items):
        gate_pair, up_pair, down_pair, table_row = items
        return expert_rows(gate_pair, up_pair, down_pair, padded[table_row])

    results = lax.map(one_expert, (gate_weight.reshape(EXPERTS, 2, D, FF_HALF),
                                   up_weight.reshape(EXPERTS, 2, D, FF_HALF),
                                   down_weight.reshape(EXPERTS, 2, FF_HALF, D),
                                   slot_table))
    picked = results[flat_ids, position].reshape(TOKENS, TOP, D).astype(jnp.float32)
    weighted = jnp.sum(picked * gate_scores[:, :, None].astype(jnp.float32), axis=1)
    local_pos = jnp.arange(TOKENS, dtype=jnp.int32) % TOK_DEV
    live_mask = local_pos < jnp.repeat(live_counts, TOK_DEV)
    return jnp.where(live_mask[:, None], weighted, jnp.zeros_like(weighted)).astype(jnp.bfloat16)
```

```python
import functools

import jax
import jax.numpy as jnp
from jax import lax
from jax.experimental import pallas as pl
from jax.experimental.pallas import tpu as pltpu
from jax.sharding import PartitionSpec as P

LANES = 128
HALF = LANES // 2


def flipped(value, mask):
    bit = 1
    while bit <= mask:
        if mask & bit:
            value = value + bit * (1 - 2 * ((value // bit) % 2))
        bit *= 2
    return value


def dense_kernel(
    planes, live_ref, tok_ref, ids_ref, score_ref, gate_hbm, up_hbm, down_hbm, out_ref,
    held, w_gate, w_up, w_down, kept, to_pair, from_pair, to_side, from_side, to_far, from_far,
    weight_sem, ag_send, ag_recv, pair_send, pair_recv, side_send, side_recv, far_send, far_recv,
):
    rows, width = tok_ref.shape
    me = lax.axis_index("expert")
    core, col, plane = me % 2, (me // 2) % 2, me // 4
    place = [flipped(plane, i) for i in range(planes)]

    def device(p, x, c):
        return (p * 2 + x) * 2 + c

    pair = device(plane, col, 1 - core)
    side = device(plane, 1 - col, core)
    far = [device(p, col, core) for p in place]

    loads = [
        pltpu.make_async_copy(src.at[0], dst, weight_sem.at[k])
        for k, (src, dst) in enumerate([(gate_hbm, w_gate), (up_hbm, w_up), (down_hbm, w_down)])
    ]
    for load in loads:
        load.start()

    def block(b):
        return pl.ds(pl.multiple_of(b * rows, rows), rows)

    held[block(me), :width] = tok_ref[...]
    lane = lax.broadcasted_iota(jnp.int32, (rows, LANES), 1)
    row = lax.broadcasted_iota(jnp.int32, (rows, LANES), 0)
    score = jnp.zeros((rows, LANES), jnp.float32)
    for k in range(ids_ref.shape[1]):
        score += jnp.where(ids_ref[:, k : k + 1] == lane % HALF, score_ref[:, k : k + 1], 0.0)
    score = jnp.where(row < live_ref[0], score, 0.0)
    high = score.astype(jnp.bfloat16).astype(jnp.float32)
    held[block(me), width:] = jnp.where(lane < HALF, high, score - high).astype(jnp.bfloat16)

    barrier = pltpu.get_barrier_semaphore()
    greeted = [pair, side] + far[1:]
    for other in greeted:
        pl.semaphore_signal(
            barrier, inc=1, device_id={"expert": other}, device_id_type=pl.DeviceIdType.MESH
        )
    pl.semaphore_wait(barrier, len(greeted))

    sent, pushed = [], []

    def send(src, dst, send_sem, recv_sem, target):
        copy = pltpu.make_async_remote_copy(
            src_ref=src, dst_ref=dst, send_sem=send_sem, recv_sem=recv_sem,
            device_id={"expert": target}, device_id_type=pl.DeviceIdType.MESH,
        )
        copy.start()
        sent.append(copy)

    def arrived(ref, recv_sem):
        pltpu.make_async_remote_copy(
            src_ref=ref, dst_ref=ref, send_sem=ag_send.at[0], recv_sem=recv_sem,
            device_id={"expert": pair}, device_id_type=pl.DeviceIdType.MESH,
        ).wait_recv()

    def push(b, target):
        where = held.at[block(b)]
        send(where, where, ag_send.at[len(pushed)], ag_recv.at[b], target)
        pushed.append(b)

    def got(b):
        arrived(held.at[block(b)], ag_recv.at[b])

    def compute(i):
        here = pl.ds(pl.multiple_of(place[i] * 4 * rows, 4 * rows), 4 * rows)
        inputs = held[here, :width]
        gate = jnp.dot(inputs, w_gate[...], preferred_element_type=jnp.float32)
        up = jnp.dot(inputs, w_up[...], preferred_element_type=jnp.float32)
        hidden = (gate / (1.0 + jnp.exp(-gate)) * up).astype(jnp.bfloat16)
        coded = held[here, width:].astype(jnp.float32)
        lanes = lax.broadcasted_iota(jnp.int32, coded.shape, 1)
        scale = jnp.sum(jnp.where(lanes % HALF == me // 2, coded, 0.0), axis=1, keepdims=True)
        if i == 0:
            loads[2].wait()
        step = 512 if width % 512 == 0 else width
        for low in range(0, width, step):
            cols = pl.ds(low, step)
            out = jnp.dot(hidden, w_down[:, cols], preferred_element_type=jnp.float32) * scale
            b00, b01, b10, b11 = [out[k * rows : (k + 1) * rows] for k in range(4)]
            mine0, theirs0 = jnp.where(core == 0, b00, b01), jnp.where(core == 0, b01, b00)
            mine1, theirs1 = jnp.where(core == 0, b10, b11), jnp.where(core == 0, b11, b10)
            kept[i, 0, :, cols] = jnp.where(col == 0, mine0, mine1)
            kept[i, 1, :, cols] = jnp.where(col == 0, mine1, mine0)
            to_pair[i, 0, :, cols] = jnp.where(col == 0, theirs0, theirs1).astype(jnp.bfloat16)
            to_pair[i, 1, :, cols] = jnp.where(col == 0, theirs1, theirs0).astype(jnp.bfloat16)
        send(to_pair.at[i], from_pair.at[i], pair_send.at[i], pair_recv.at[i], pair)

    def join_pair(i):
        arrived(from_pair.at[i], pair_recv.at[i])
        to_side[i] = (kept[i, 1] + from_pair[i, 1].astype(jnp.float32)).astype(jnp.bfloat16)
        send(to_side.at[i], from_side.at[i], side_send.at[i], side_recv.at[i], side)

    def join_side(i):
        arrived(from_side.at[i], side_recv.at[i])
        total = kept[i, 0] + from_pair[i, 0].astype(jnp.float32)
        return total + from_side[i].astype(jnp.float32)

    def send_far(i):
        to_far[i] = join_side(i).astype(jnp.bfloat16)
        send(to_far.at[i], from_far.at[i], far_send.at[i], far_recv.at[i], far[i])

    push(me, side)
    push(me, pair)
    for i in range(1, planes):
        push(me, far[i])

    for i in range(planes):
        if i + 1 < planes:
            got(far[i + 1])
            push(far[i + 1], side)
            push(far[i + 1], pair)
        got(device(place[i], 1 - col, core))
        push(device(place[i], 1 - col, core), pair)
        got(device(place[i], col, 1 - core))
        got(device(place[i], 1 - col, 1 - core))
        if i == 0:
            loads[0].wait()
            loads[1].wait()
        compute(i)
        if i >= 2:
            join_pair(i - 1)
        if i >= 3:
            send_far(i - 2)
    if planes > 1:
        join_pair(planes - 1)
    join_pair(0)
    for i in range(max(1, planes - 2), planes):
        send_far(i)
    total = join_side(0)
    for i in range(1, planes):
        arrived(from_far.at[i], far_recv.at[i])
        total += from_far[i].astype(jnp.float32)
    out_ref[...] = total.astype(jnp.bfloat16)
    for copy in sent:
        copy.wait_send()


def dense_shards(tokens, live_counts, expert_ids, gate_scores, gate_weight, up_weight, down_weight):
    rows, width = tokens.shape
    units = gate_weight.shape[2]
    devices = lax.axis_size("expert")
    planes = devices // 4
    block = (rows, width)
    vmem = pl.BlockSpec(memory_space=pltpu.VMEM)
    hbm = pl.BlockSpec(memory_space=pl.ANY)
    dma = pltpu.SemaphoreType.DMA
    return pl.pallas_call(
        functools.partial(dense_kernel, planes),
        out_shape=jax.ShapeDtypeStruct(block, jnp.bfloat16),
        in_specs=[pl.BlockSpec(memory_space=pltpu.SMEM), vmem, vmem, vmem, hbm, hbm, hbm],
        out_specs=vmem,
        scratch_shapes=[
            pltpu.VMEM((devices * rows, width + LANES), jnp.bfloat16),
            pltpu.VMEM((width, units), jnp.bfloat16),
            pltpu.VMEM((width, units), jnp.bfloat16),
            pltpu.VMEM((units, width), jnp.bfloat16),
            pltpu.VMEM((planes, 2) + block, jnp.float32),
            pltpu.VMEM((planes, 2) + block, jnp.bfloat16),
            pltpu.VMEM((planes, 2) + block, jnp.bfloat16),
            pltpu.VMEM((planes,) + block, jnp.bfloat16),
            pltpu.VMEM((planes,) + block, jnp.bfloat16),
            pltpu.VMEM((planes,) + block, jnp.bfloat16),
            pltpu.VMEM((planes,) + block, jnp.bfloat16),
            dma((3,)),
            dma((4 * planes,)),
            dma((devices,)),
            dma((planes,)),
            dma((planes,)),
            dma((planes,)),
            dma((planes,)),
            dma((planes,)),
            dma((planes,)),
        ],
        compiler_params=pltpu.CompilerParams(
            collective_id=0, has_side_effects=True, vmem_limit_bytes=60 * 1024 * 1024
        ),
    )(live_counts, tokens, expert_ids, gate_scores, gate_weight, up_weight, down_weight)


def partner_2(block, axis, apart):
    count = lax.axis_size(axis)
    route = []
    for low in range(count):
        high = low | 1 << apart
        if high != low and high < count:
            route += [(low, high), (high, low)]
    return lax.ppermute(block, axis, route)


def expert_rows(slot_rows, gate_weight, up_weight, down_weight):
    model_width = slot_rows.shape[-1]
    flat_rows = slot_rows.reshape(-1, model_width)
    gate_act = jnp.dot(flat_rows, gate_weight[0], preferred_element_type=jnp.float32)
    up_act = jnp.dot(flat_rows, up_weight[0], preferred_element_type=jnp.float32)
    hidden = (jax.nn.silu(gate_act) * up_act).astype(jnp.bfloat16)
    partial_value = jnp.dot(hidden, down_weight[0], preferred_element_type=jnp.float32)
    return partial_value.reshape(slot_rows.shape)


def packed_shards(tokens, live_counts, expert_ids, gate_scores, gate_weight, up_weight, down_weight):
    tok_dev, model_width = tokens.shape
    top_count = expert_ids.shape[1]
    devices = lax.axis_size("expert")
    experts = devices // 2
    capacity = 2 * tok_dev * top_count // experts
    half_width = model_width // 2
    parity = lax.axis_index("expert") % 2
    flat_ids = expert_ids.reshape(-1)
    onehot = (flat_ids[:, None] == jnp.arange(experts, dtype=jnp.int32)[None, :]).astype(jnp.int32)
    earlier = jnp.cumsum(onehot, axis=0) - onehot
    slot_index = jnp.sum(earlier * onehot, axis=1)
    target = flat_ids * capacity + slot_index
    placing = (jnp.arange(experts * capacity, dtype=jnp.int32)[:, None] == target[None, :]).astype(
        jnp.int32
    )
    placing = (
        placing.reshape(experts * capacity, tok_dev, top_count).sum(axis=2).astype(jnp.bfloat16)
    )
    packed = jnp.dot(placing, tokens, preferred_element_type=jnp.float32).astype(jnp.bfloat16)
    outgoing = packed.reshape(devices, capacity // 2, model_width)
    slot_rows = lax.all_to_all(outgoing, "expert", split_axis=0, concat_axis=0, tiled=True)
    partner = partner_2(slot_rows, "expert", 0)
    count = slot_rows.shape[1]
    run_slot_rows = jnp.concatenate([slot_rows, partner], axis=1)
    paired = expert_rows(run_slot_rows, gate_weight, up_weight, down_weight)
    own_part = paired[:, :count]
    partner_part = paired[:, count:]
    lower_half = jnp.where(parity == 0, own_part, partner_part)
    second = jnp.where(parity == 0, partner_part, own_part)
    stacked = jnp.stack([lower_half, second], axis=1)
    partial_value = stacked.reshape(devices, capacity, model_width)
    partner_sum = partner_2(partial_value, "expert", 0)
    summed = partial_value + partner_sum
    own_part = lax.dynamic_slice_in_dim(summed, parity * half_width, half_width, 2).astype(
        jnp.bfloat16
    )
    returned = lax.all_to_all(own_part, "expert", split_axis=0, concat_axis=0, tiled=True)
    returned = returned.reshape(experts, 2, capacity, half_width)
    picked = returned[flat_ids, :, slot_index, :]
    picked = picked.reshape(tok_dev, top_count, model_width).astype(jnp.float32)
    weighted = jnp.sum(picked * gate_scores[:, :, None], axis=1)
    live_mask = jnp.arange(tok_dev, dtype=jnp.int32) < live_counts[0]
    return jnp.where(live_mask[:, None], weighted, jnp.zeros_like(weighted)).astype(jnp.bfloat16)


def shards(tokens, live_counts, expert_ids, gate_scores, gate_weight, up_weight, down_weight):
    args = (tokens, live_counts, expert_ids, gate_scores, gate_weight, up_weight, down_weight)
    tok_dev, top_count = expert_ids.shape
    devices = lax.axis_size("expert")
    experts = devices // 2
    planes = devices // 4
    dense = 2 * tok_dev * top_count // experts >= tok_dev
    if dense and devices % 4 == 0 and planes & (planes - 1) == 0 and experts <= HALF:
        return dense_shards(*args)
    return packed_shards(*args)


def solution(mesh):
    in_specs = (
        P(("groups", "expert"), None),
        P(("groups", "expert")),
        P(("groups", "expert"), None),
        P(("groups", "expert"), None),
        P("expert", None, None),
        P("expert", None, None),
        P("expert", None, None),
    )
    out_specs = P(("groups", "expert"), None)
    return jax.shard_map(shards, mesh=mesh, in_specs=in_specs, out_specs=out_specs, check_vma=False)
```

```python
import functools

import jax
import jax.numpy as jnp
from jax import lax
from jax.experimental import pallas as pl
from jax.experimental.pallas import tpu as pltpu
from jax.sharding import PartitionSpec as P

LANES = 128
HALF = LANES // 2


def flipped(value, mask):
    bit = 1
    while bit <= mask:
        if mask & bit:
            value = value + bit * (1 - 2 * ((value // bit) % 2))
        bit *= 2
    return value


def dense_kernel(
    planes, live_ref, tok_ref, ids_ref, score_ref, gate_hbm, up_hbm, down_hbm, out_ref,
    held, w_gate, w_up, w_down, kept, to_pair, from_pair, to_side, from_side, to_far, from_far,
    weight_sem, ag_send, ag_recv, pair_send, pair_recv, side_send, side_recv, far_send, far_recv,
):
    rows, width = tok_ref.shape
    me = lax.axis_index("expert")
    core, col, plane = me % 2, (me // 2) % 2, me // 4
    place = [flipped(plane, i) for i in range(planes)]

    def device(p, x, c):
        return (p * 2 + x) * 2 + c

    pair = device(plane, col, 1 - core)
    side = device(plane, 1 - col, core)
    far = [device(p, col, core) for p in place]

    loads = [
        pltpu.make_async_copy(src.at[0], dst, weight_sem.at[k])
        for k, (src, dst) in enumerate([(gate_hbm, w_gate), (up_hbm, w_up), (down_hbm, w_down)])
    ]
    for load in loads:
        load.start()

    def block(b):
        return pl.ds(pl.multiple_of(b * rows, rows), rows)

    held[block(me), :width] = tok_ref[...]
    lane = lax.broadcasted_iota(jnp.int32, (rows, LANES), 1)
    row = lax.broadcasted_iota(jnp.int32, (rows, LANES), 0)
    score = jnp.zeros((rows, LANES), jnp.float32)
    across = lax.broadcasted_iota(jnp.int32, (rows, rows), 1)
    down = lax.broadcasted_iota(jnp.int32, (rows, rows), 0)

    def column(line):
        return jnp.sum(jnp.where(across == down, line, jnp.zeros_like(line)), axis=1, keepdims=True)

    for k in range(ids_ref.shape[0]):
        named = column(ids_ref[k : k + 1, :].astype(jnp.float32)).astype(jnp.int32)
        score += jnp.where(named == lane % HALF, column(score_ref[k : k + 1, :]), 0.0)
    score = jnp.where(row < live_ref[0], score, 0.0)
    high = score.astype(jnp.bfloat16).astype(jnp.float32)
    held[block(me), width:] = jnp.where(lane < HALF, high, score - high).astype(jnp.bfloat16)

    barrier = pltpu.get_barrier_semaphore()
    greeted = [pair, side] + far[1:]
    for other in greeted:
        pl.semaphore_signal(
            barrier, inc=1, device_id={"expert": other}, device_id_type=pl.DeviceIdType.MESH
        )
    pl.semaphore_wait(barrier, len(greeted))

    sent, pushed = [], []

    def send(src, dst, send_sem, recv_sem, target):
        copy = pltpu.make_async_remote_copy(
            src_ref=src, dst_ref=dst, send_sem=send_sem, recv_sem=recv_sem,
            device_id={"expert": target}, device_id_type=pl.DeviceIdType.MESH,
        )
        copy.start()
        sent.append(copy)

    def arrived(ref, recv_sem):
        pltpu.make_async_remote_copy(
            src_ref=ref, dst_ref=ref, send_sem=ag_send.at[0], recv_sem=recv_sem,
            device_id={"expert": pair}, device_id_type=pl.DeviceIdType.MESH,
        ).wait_recv()

    def push(b, target):
        where = held.at[block(b)]
        send(where, where, ag_send.at[len(pushed)], ag_recv.at[b], target)
        pushed.append(b)

    def got(b):
        arrived(held.at[block(b)], ag_recv.at[b])

    def compute(i):
        here = pl.ds(pl.multiple_of(place[i] * 4 * rows, 4 * rows), 4 * rows)
        inputs = held[here, :width]
        gate = jnp.dot(inputs, w_gate[...], preferred_element_type=jnp.float32)
        up = jnp.dot(inputs, w_up[...], preferred_element_type=jnp.float32)
        hidden = (gate / (1.0 + jnp.exp(-gate)) * up).astype(jnp.bfloat16)
        coded = held[here, width:].astype(jnp.float32)
        lanes = lax.broadcasted_iota(jnp.int32, coded.shape, 1)
        scale = jnp.sum(jnp.where(lanes % HALF == me // 2, coded, 0.0), axis=1, keepdims=True)
        if i == 0:
            loads[2].wait()
        step = 512 if width % 512 == 0 else width
        for low in range(0, width, step):
            cols = pl.ds(low, step)
            out = jnp.dot(hidden, w_down[:, cols], preferred_element_type=jnp.float32) * scale
            b00, b01, b10, b11 = [out[k * rows : (k + 1) * rows] for k in range(4)]
            mine0, theirs0 = jnp.where(core == 0, b00, b01), jnp.where(core == 0, b01, b00)
            mine1, theirs1 = jnp.where(core == 0, b10, b11), jnp.where(core == 0, b11, b10)
            kept[i, 0, :, cols] = jnp.where(col == 0, mine0, mine1)
            kept[i, 1, :, cols] = jnp.where(col == 0, mine1, mine0)
            to_pair[i, 0, :, cols] = jnp.where(col == 0, theirs0, theirs1).astype(jnp.bfloat16)
            to_pair[i, 1, :, cols] = jnp.where(col == 0, theirs1, theirs0).astype(jnp.bfloat16)
        send(to_pair.at[i], from_pair.at[i], pair_send.at[i], pair_recv.at[i], pair)

    def join_pair(i):
        arrived(from_pair.at[i], pair_recv.at[i])
        to_side[i] = (kept[i, 1] + from_pair[i, 1].astype(jnp.float32)).astype(jnp.bfloat16)
        send(to_side.at[i], from_side.at[i], side_send.at[i], side_recv.at[i], side)

    def join_side(i):
        arrived(from_side.at[i], side_recv.at[i])
        total = kept[i, 0] + from_pair[i, 0].astype(jnp.float32)
        return total + from_side[i].astype(jnp.float32)

    def send_far(i):
        to_far[i] = join_side(i).astype(jnp.bfloat16)
        send(to_far.at[i], from_far.at[i], far_send.at[i], far_recv.at[i], far[i])

    push(me, side)
    push(me, pair)
    for i in range(1, planes):
        push(me, far[i])

    for i in range(planes):
        if i + 1 < planes:
            got(far[i + 1])
            push(far[i + 1], side)
            push(far[i + 1], pair)
        got(device(place[i], 1 - col, core))
        push(device(place[i], 1 - col, core), pair)
        got(device(place[i], col, 1 - core))
        got(device(place[i], 1 - col, 1 - core))
        if i == 0:
            loads[0].wait()
            loads[1].wait()
        compute(i)
        if i >= 2:
            join_pair(i - 1)
        if i >= 3:
            send_far(i - 2)
    if planes > 1:
        join_pair(planes - 1)
    join_pair(0)
    for i in range(max(1, planes - 2), planes):
        send_far(i)
    total = join_side(0)
    for i in range(1, planes):
        arrived(from_far.at[i], far_recv.at[i])
        total += from_far[i].astype(jnp.float32)
    out_ref[...] = total.astype(jnp.bfloat16)
    for copy in sent:
        copy.wait_send()


def dense_shards(tokens, live_counts, expert_ids, gate_scores, gate_weight, up_weight, down_weight):
    rows, width = tokens.shape
    units = gate_weight.shape[2]
    devices = lax.axis_size("expert")
    planes = devices // 4
    block = (rows, width)
    vmem = pl.BlockSpec(memory_space=pltpu.VMEM)
    hbm = pl.BlockSpec(memory_space=pl.ANY)
    dma = pltpu.SemaphoreType.DMA
    return pl.pallas_call(
        functools.partial(dense_kernel, planes),
        out_shape=jax.ShapeDtypeStruct(block, jnp.bfloat16),
        in_specs=[pl.BlockSpec(memory_space=pltpu.SMEM), vmem, vmem, vmem, hbm, hbm, hbm],
        out_specs=vmem,
        scratch_shapes=[
            pltpu.VMEM((devices * rows, width + LANES), jnp.bfloat16),
            pltpu.VMEM((width, units), jnp.bfloat16),
            pltpu.VMEM((width, units), jnp.bfloat16),
            pltpu.VMEM((units, width), jnp.bfloat16),
            pltpu.VMEM((planes, 2) + block, jnp.float32),
            pltpu.VMEM((planes, 2) + block, jnp.bfloat16),
            pltpu.VMEM((planes, 2) + block, jnp.bfloat16),
            pltpu.VMEM((planes,) + block, jnp.bfloat16),
            pltpu.VMEM((planes,) + block, jnp.bfloat16),
            pltpu.VMEM((planes,) + block, jnp.bfloat16),
            pltpu.VMEM((planes,) + block, jnp.bfloat16),
            dma((3,)),
            dma((4 * planes,)),
            dma((devices,)),
            dma((planes,)),
            dma((planes,)),
            dma((planes,)),
            dma((planes,)),
            dma((planes,)),
            dma((planes,)),
        ],
        compiler_params=pltpu.CompilerParams(
            collective_id=0, has_side_effects=True, vmem_limit_bytes=60 * 1024 * 1024
        ),
    )(live_counts, tokens, expert_ids.T, gate_scores.T, gate_weight, up_weight, down_weight)


def partner_2(block, axis, apart):
    count = lax.axis_size(axis)
    route = []
    for low in range(count):
        high = low | 1 << apart
        if high != low and high < count:
            route += [(low, high), (high, low)]
    return lax.ppermute(block, axis, route)


def expert_rows(slot_rows, gate_weight, up_weight, down_weight):
    model_width = slot_rows.shape[-1]
    flat_rows = slot_rows.reshape(-1, model_width)
    gate_act = jnp.dot(flat_rows, gate_weight[0], preferred_element_type=jnp.float32)
    up_act = jnp.dot(flat_rows, up_weight[0], preferred_element_type=jnp.float32)
    hidden = (jax.nn.silu(gate_act) * up_act).astype(jnp.bfloat16)
    partial_value = jnp.dot(hidden, down_weight[0], preferred_element_type=jnp.float32)
    return partial_value.reshape(slot_rows.shape)


def packed_shards(tokens, live_counts, expert_ids, gate_scores, gate_weight, up_weight, down_weight):
    tok_dev, model_width = tokens.shape
    top_count = expert_ids.shape[1]
    devices = lax.axis_size("expert")
    experts = devices // 2
    capacity = 2 * tok_dev * top_count // experts
    half_width = model_width // 2
    parity = lax.axis_index("expert") % 2
    flat_ids = expert_ids.reshape(-1)
    onehot = (flat_ids[:, None] == jnp.arange(experts, dtype=jnp.int32)[None, :]).astype(jnp.int32)
    earlier = jnp.cumsum(onehot, axis=0) - onehot
    slot_index = jnp.sum(earlier * onehot, axis=1)
    target = flat_ids * capacity + slot_index
    placing = (jnp.arange(experts * capacity, dtype=jnp.int32)[:, None] == target[None, :]).astype(
        jnp.int32
    )
    placing = (
        placing.reshape(experts * capacity, tok_dev, top_count).sum(axis=2).astype(jnp.bfloat16)
    )
    packed = jnp.dot(placing, tokens, preferred_element_type=jnp.float32).astype(jnp.bfloat16)
    outgoing = packed.reshape(devices, capacity // 2, model_width)
    slot_rows = lax.all_to_all(outgoing, "expert", split_axis=0, concat_axis=0, tiled=True)
    partner = partner_2(slot_rows, "expert", 0)
    count = slot_rows.shape[1]
    run_slot_rows = jnp.concatenate([slot_rows, partner], axis=1)
    paired = expert_rows(run_slot_rows, gate_weight, up_weight, down_weight)
    own_part = paired[:, :count]
    partner_part = paired[:, count:]
    lower_half = jnp.where(parity == 0, own_part, partner_part)
    second = jnp.where(parity == 0, partner_part, own_part)
    stacked = jnp.stack([lower_half, second], axis=1)
    partial_value = stacked.reshape(devices, capacity, model_width)
    partner_sum = partner_2(partial_value, "expert", 0)
    summed = partial_value + partner_sum
    own_part = lax.dynamic_slice_in_dim(summed, parity * half_width, half_width, 2).astype(
        jnp.bfloat16
    )
    returned = lax.all_to_all(own_part, "expert", split_axis=0, concat_axis=0, tiled=True)
    returned = returned.reshape(experts, 2, capacity, half_width)
    picked = returned[flat_ids, :, slot_index, :]
    picked = picked.reshape(tok_dev, top_count, model_width).astype(jnp.float32)
    weighted = jnp.sum(picked * gate_scores[:, :, None], axis=1)
    live_mask = jnp.arange(tok_dev, dtype=jnp.int32) < live_counts[0]
    return jnp.where(live_mask[:, None], weighted, jnp.zeros_like(weighted)).astype(jnp.bfloat16)


def shards(tokens, live_counts, expert_ids, gate_scores, gate_weight, up_weight, down_weight):
    args = (tokens, live_counts, expert_ids, gate_scores, gate_weight, up_weight, down_weight)
    tok_dev, top_count = expert_ids.shape
    devices = lax.axis_size("expert")
    experts = devices // 2
    planes = devices // 4
    dense = 2 * tok_dev * top_count // experts >= tok_dev
    if dense and devices % 4 == 0 and planes & (planes - 1) == 0 and experts <= HALF:
        return dense_shards(*args)
    return packed_shards(*args)


def solution(mesh):
    in_specs = (
        P(("groups", "expert"), None),
        P(("groups", "expert")),
        P(("groups", "expert"), None),
        P(("groups", "expert"), None),
        P("expert", None, None),
        P("expert", None, None),
        P("expert", None, None),
    )
    out_specs = P(("groups", "expert"), None)
    return jax.shard_map(shards, mesh=mesh, in_specs=in_specs, out_specs=out_specs, check_vma=False)
```
